256 devices in a mesh: scan: 32 (over z, y), lat: 8 (over x, core).
Axes of the slice: x: 4, y: 4, z: 8, core: 2. Of those that a mesh axis runs over, the one named last changes fastest.
Arguments:
- observed: bfloat16 [384, 512, 512], P('scan', 'lat'), may hold values from 0.099609375 to 4
- estimate: float32 [384, 512, 512], P('scan', 'lat'), may hold values from 0.1 to 4
- column_weights: float32 [512, 512], replicated, may hold values from 0 to 0.5, as said below
- plane_taps: float32 [7], replicated, may hold values from 0.1 to 1
- row_taps: float32 [7], replicated, may hold values from 0.1 to 1
- shear_planes: int32 [512], replicated, may hold values from 1 to 383, as said below
Outputs:
- deskewed: float32 [384, 512, 512], P('scan', 'lat')
The draws below stay inside these ranges and needn't reach their ends.
Inputs may be any that keep to these rules, and one draw needn't show every extreme that they name: `shear_planes`: never falls from one column to the next; the first column's offset is 1 and the last column's is 383. `column_weights`: zero more than 8 columns away from the diagonal, positive within.
All inputs are finite; a program needn't handle non-finite values.
Results may differ from the reference program's by a relative error of at most 0.0003.
Values sent between devices are 32-bit elements; how exact they have to be, the bound alone decides.
A program may use at most 64 MiB of HBM per device.

```python
import math
import jax
import jax.numpy as jnp
from jax import lax

PD = 12
X = 512
PLANE_HALF = 3
ROW_HALF = 3
SKEW = 2
BAND = 8
P_SIZE = 384
Y = 512


def draw_column_weights(key, part):
    values = jnp.exp(jax.random.uniform(key, (X, X), jnp.float32, jnp.log(0.05), jnp.log(0.5)))
    row_ids = jnp.arange(X)[:, None]
    col_ids = jnp.arange(X)[None, :]
    return jnp.where(jnp.abs(row_ids - col_ids) <= BAND, values, 0.0).astype(jnp.float32)


def draw_shear_planes(key, part):
    step_key = jax.random.fold_in(key, 11)
    first_key = jax.random.fold_in(key, 23)
    steps = jax.random.randint(step_key, (X,), 0, 2 * P_SIZE)
    climbed = (jnp.cumsum(steps) - steps[0]) // X
    first = jax.random.randint(first_key, (), 1, PD)
    shaped = jnp.maximum(jnp.minimum(climbed, P_SIZE - 1), first)
    col_ids = jnp.arange(X)
    shaped = jnp.where(col_ids == 0, 1, shaped)
    return jnp.where(col_ids == X - 1, P_SIZE - 1, shaped).astype(jnp.int32)


def level_of(key, dims, pieces, low, top_value):
    loudness = 1.0
    for dim, shards_of in pieces:
        heights = jax.random.uniform(jax.random.fold_in(jax.random.fold_in(key, 6), dim), (shards_of,), jnp.float32, low / len(pieces), top_value / len(pieces))
        loudness = loudness * jnp.repeat(jnp.exp(heights), dims[dim] // shards_of).reshape((-1,) + (1,) * (len(dims) - 1 - dim))
    return loudness


def setup_inputs(seed: int = 0) -> dict:
    key_of = jax.random.split(jax.random.key(seed), 7)
    observed = jnp.clip(jnp.exp(math.log(4.0) - 3.6927934 * jax.random.uniform(key_of[0], (P_SIZE, Y, X), jnp.float32) ** level_of(key_of[0], (P_SIZE, Y, X), ((0, 32), (1, 8)), -0.2, 0.2)), 0.099609375, 4.0).astype(jnp.bfloat16)
    estimate = jnp.clip(jnp.exp(math.log(4.0) - 3.6888794 * jax.random.uniform(key_of[1], (P_SIZE, Y, X), jnp.float32) ** level_of(key_of[1], (P_SIZE, Y, X), ((0, 32), (1, 8)), -0.2, 0.2)), 0.1, 4.0)
    column_weights = draw_column_weights(jax.random.fold_in(key_of[6], 71), 0)
    plane_taps = jnp.clip(jnp.exp(jax.random.uniform(key_of[3], (2 * PLANE_HALF + 1,), jnp.float32, math.log(0.1), math.log(1.0))), 0.1, 1.0)
    row_taps = jnp.clip(jnp.exp(jax.random.uniform(key_of[4], (2 * ROW_HALF + 1,), jnp.float32, math.log(0.1), math.log(1.0))), 0.1, 1.0)
    shear_planes = draw_shear_planes(jax.random.fold_in(key_of[6], 71), 0)
    return {"observed": observed, "estimate": estimate, "column_weights": column_weights, "plane_taps": plane_taps, "row_taps": row_taps, "shear_planes": shear_planes}


def column_mix(field, matrix):
    flat = field.reshape(-1, matrix.shape[0])
    mixed = jnp.dot(flat, matrix, precision=lax.Precision.HIGHEST, preferred_element_type=jnp.float32)
    return mixed.reshape(field.shape)


def row_pass(padded, kernel, direction):
    halfwidth = (kernel.shape[0] - 1) // 2
    row_count = padded.shape[1] - 2 * halfwidth
    summed = jnp.zeros((padded.shape[0], row_count, padded.shape[2]), jnp.float32)
    for offset in range(-halfwidth, halfwidth + 1):
        begin = halfwidth + direction * offset
        summed = summed + kernel[offset + halfwidth] * padded[:, begin:begin + row_count, :]
    return summed


def plane_pass(padded, kernel, direction):
    halfwidth = (kernel.shape[0] - 1) // 2
    plane_count = padded.shape[0] - 2 * halfwidth
    column_count = padded.shape[2]
    widened = jnp.pad(padded, ((0, 0), (0, 0), (halfwidth * SKEW, halfwidth * SKEW)))
    summed = jnp.zeros((plane_count, padded.shape[1], column_count), jnp.float32)
    for offset in range(-halfwidth, halfwidth + 1):
        begin = halfwidth + direction * offset
        column_start = halfwidth * SKEW - direction * offset * SKEW
        summed = summed + kernel[offset + halfwidth] * widened[begin:begin + plane_count, :, column_start:column_start + column_count]
    return summed


def pad_rows(field):
    return jnp.pad(field, ((0, 0), (ROW_HALF, ROW_HALF), (0, 0)))


def pad_planes(field):
    return jnp.pad(field, ((PLANE_HALF, PLANE_HALF), (0, 0), (0, 0)))


def reference(observed, estimate, column_weights, plane_taps, row_taps, shear_planes):
    mixed_cols = column_mix(estimate, column_weights)
    row_blur = row_pass(pad_rows(mixed_cols), row_taps, 1)
    blurred = plane_pass(pad_planes(row_blur), plane_taps, 1)
    quotient = observed.astype(jnp.float32) / blurred
    back_planes = plane_pass(pad_planes(quotient), plane_taps, -1)
    back_rows = row_pass(pad_rows(back_planes), row_taps, -1)
    correction = column_mix(back_rows, column_weights.T)
    updated = estimate * correction
    source_ids = jnp.arange(P_SIZE, dtype=jnp.int32)[:, None] - shear_planes[None, :]
    taken = jnp.take_along_axis(updated, jnp.maximum(source_ids, 0)[:, None, :], axis=0)
    return jnp.where((source_ids >= 0)[:, None, :], taken, 0.0)
```

```python
import functools

import jax
import jax.numpy as jnp
from jax import lax
from jax.experimental import pallas as pl
from jax.experimental.pallas import tpu as pltpu
from jax.sharding import PartitionSpec as P

MESH = pl.DeviceIdType.MESH
F32 = jnp.float32
BF16 = jnp.bfloat16
PLANES = 12
PAIRS = 6
ROWS = 64
COLS = 512
LANES = 128
TILES = COLS // LANES
PAD = 8


def split(x):
    hi = x.astype(BF16)
    return hi, (x - hi.astype(F32)).astype(BF16)


def dot(a, b):
    return jnp.dot(a, b, preferred_element_type=F32)


def lane_ids(rows):
    return lax.broadcasted_iota(jnp.int32, (rows, LANES), 1)


def half_roll(x):
    return pltpu.roll(x, ROWS, 1)


def row_matrix(taps, flip):
    line = lax.broadcasted_iota(jnp.int32, (LANES, LANES), 0)
    column = lax.broadcasted_iota(jnp.int32, (LANES, LANES), 1)
    same = (line >= ROWS) == (column >= ROWS)
    row = line & (ROWS - 1)
    target = column & (ROWS - 1)
    far = jnp.where(row < ROWS // 2, row + ROWS, row - ROWS)
    own = jnp.zeros((LANES, LANES), F32)
    edge = jnp.zeros((LANES, LANES), F32)
    for b in range(-3, 4):
        tap = taps[3 - b] if flip else taps[b + 3]
        own = jnp.where(same & (row - target == b), tap, own)
        edge = jnp.where(same & (far - target == b), tap, edge)
    return jnp.concatenate([own, edge], axis=0)


def kernel(
    n,
    nl,
    obs_h,
    est_h,
    w_h,
    pt,
    rt,
    sh,
    out_h,
    obs,
    est,
    w,
    est_t,
    obs_t,
    wmat,
    tmat,
    edge_s,
    edge_r,
    rim_s,
    rim_r,
    hc,
    zf,
    bp,
    rhi,
    rlo,
    upd,
    got,
    lined,
    back,
    fin,
    outv,
    in_sem,
    edge_ss,
    edge_rs,
    rim_ss,
    rim_rs,
    a_ss,
    a_rs,
    b_ss,
    b_rs,
    own_sem,
):
    group = COLS // n
    pitch = 2 * PLANES * n + 9
    me = lax.axis_index("scan")
    lat = lax.axis_index("lat")
    s_prev, s_next = lax.rem(me + n - 1, n), lax.rem(me + 1, n)
    l_prev, l_next = lax.rem(lat + nl - 1, nl), lax.rem(lat + 1, nl)

    barrier = pltpu.get_barrier_semaphore()

    def greet(k, carry):
        pl.semaphore_signal(barrier, inc=1, device_id={"scan": lax.rem(me + k, n), "lat": lat}, device_id_type=MESH)
        return carry

    for other in (l_prev, l_next):
        pl.semaphore_signal(barrier, inc=1, device_id={"scan": me, "lat": other}, device_id_type=MESH)
    lax.fori_loop(1, n, greet, 0)

    loads = [
        pltpu.make_async_copy(est_h, est, in_sem.at[0]),
        pltpu.make_async_copy(w_h, w, in_sem.at[1]),
        pltpu.make_async_copy(obs_h, obs, in_sem.at[2]),
    ]
    for load in loads:
        load.start()

    def send_edges(stage, field):
        def chunk(i, carry):
            at = pl.ds(pl.multiple_of(i * 64, 64), 64)
            lane = lane_ids(64)
            packed = jnp.zeros((64, LANES), F32)
            for m in range(PAIRS):
                x = field[m, at, :]
                moved = pltpu.roll(x, 6 * m, 1) if m else x
                window = (lane + (3 + ROWS - 6 * m)) & (ROWS - 1)
                packed = jnp.where(window < 6, moved, packed)
            edge_s[stage, at, :] = packed
            return carry

        lax.fori_loop(0, COLS // 64, chunk, 0)

    def edge_copies(stage):
        return [
            pltpu.make_async_remote_copy(
                src_ref=edge_s.at[stage],
                dst_ref=edge_r.at[stage, i],
                send_sem=edge_ss.at[stage, i],
                recv_sem=edge_rs.at[stage, i],
                device_id={"scan": me, "lat": other},
                device_id_type=MESH,
            )
            for i, other in ((0, l_next), (1, l_prev))
        ]

    def join_edges(stage):
        def chunk(i, carry):
            at = pl.ds(pl.multiple_of(i * 64, 64), 64)
            spot = (lane_ids(64) + 3) & (ROWS - 1)
            first = lax.rem(spot, 6) < 3
            before = jnp.where(lat > 0, edge_r[stage, 0, at, :], 0.0)
            after = jnp.where(lat < nl - 1, edge_r[stage, 1, at, :], 0.0)
            hc[at, :] = jnp.where(first, before, after)
            return carry

        lax.fori_loop(0, COLS // 64, chunk, 0)

    def row_pass(stage, field):
        def chunk(i, carry):
            at = pl.ds(pl.multiple_of(i * LANES, LANES), LANES)
            edges = hc[at, :]
            for m in range(PAIRS):
                moved = pltpu.roll(edges, LANES - 6 * m, 1) if m else edges
                hi, lo = split(jnp.concatenate([field[m, at, :], moved], axis=1))
                t_hi, t_lo = tmat[stage, 0], tmat[stage, 1]
                y_hi, y_lo = split(dot(hi, t_hi) + dot(lo, t_hi) + dot(hi, t_lo))
                rhi[at, m * LANES : (m + 1) * LANES] = y_hi
                rlo[at, m * LANES : (m + 1) * LANES] = y_lo
            return carry

        lax.fori_loop(0, TILES, chunk, 0)

    def mix(stage, store):
        for b in range(TILES):
            k0, k1 = max(0, b - 1) * LANES, min(TILES, b + 2) * LANES
            block = slice(b * LANES, (b + 1) * LANES)
            w_hi, w_lo = wmat[stage, 0, block, k0:k1], wmat[stage, 1, block, k0:k1]
            for pair in range(PAIRS // 2):
                lanes = slice(pair * 2 * LANES, (pair + 1) * 2 * LANES)
                x_hi, x_lo = rhi[k0:k1, lanes], rlo[k0:k1, lanes]
                y = dot(w_hi, x_hi) + dot(w_hi, x_lo) + dot(w_lo, x_hi)
                store(2 * pair, b, y[:, :LANES])
                store(2 * pair + 1, b, y[:, LANES:])

    def pack_rims(stage):
        def chunk(i, carry):
            lane = lane_ids(64)
            low = lane < ROWS
            r = pl.multiple_of(i * 64, 64)
            at = pl.ds(r + PAD, 64)
            rim_s[stage, 0, pl.ds(r, 64), :] = jnp.where(low, half_roll(zf[6, at, :]), zf[7, at, :])
            rim_s[stage, 1, pl.ds(r, 64), :] = jnp.where(low, zf[3, at, :], half_roll(zf[4, at, :]))
            return carry

        lax.fori_loop(0, COLS // 64, chunk, 0)

        def rest(i, carry):
            low = lane_ids(64) < ROWS
            r = pl.multiple_of(i * 64, 64)
            at, far = pl.ds(r + PAD, 64), pl.ds(r + PAD + COLS // 2, 64)
            rim_s[stage, 0, pl.ds(r + COLS, 64), :] = jnp.where(low, half_roll(zf[8, at, :]), zf[8, far, :])
            rim_s[stage, 1, pl.ds(r + COLS, 64), :] = jnp.where(low, zf[5, at, :], half_roll(zf[5, far, :]))
            return carry

        lax.fori_loop(0, COLS // 128, rest, 0)

    def rim_copies(stage):
        return [
            pltpu.make_async_remote_copy(
                src_ref=rim_s.at[stage, i],
                dst_ref=rim_r.at[stage, i],
                send_sem=rim_ss.at[stage, i],
                recv_sem=rim_rs.at[stage, i],
                device_id={"scan": other, "lat": lat},
                device_id_type=MESH,
            )
            for i, other in ((0, s_next), (1, s_prev))
        ]

    def unpack_rims(stage):
        def chunk(i, carry):
            low = lane_ids(64) < ROWS
            r = pl.multiple_of(i * 64, 64)
            at = pl.ds(r + PAD, 64)
            before = jnp.where(me > 0, rim_r[stage, 0, pl.ds(r, 64), :], 0.0)
            after = jnp.where(me < n - 1, rim_r[stage, 1, pl.ds(r, 64), :], 0.0)
            zf[0, at, :] = jnp.where(low, before, half_roll(zf[6, at, :]))
            zf[1, at, :] = half_roll(jnp.where(low, zf[7, at, :], before))
            zf[9, at, :] = half_roll(jnp.where(low, after, zf[3, at, :]))
            zf[10, at, :] = jnp.where(low, half_roll(zf[4, at, :]), after)
            return carry

        lax.fori_loop(0, COLS // 64, chunk, 0)

        def rest(i, carry):
            low = lane_ids(64) < ROWS
            r = pl.multiple_of(i * 64, 64)
            at, far = pl.ds(r + PAD, 64), pl.ds(r + PAD + COLS // 2, 64)
            before = jnp.where(me > 0, rim_r[stage, 0, pl.ds(r + COLS, 64), :], 0.0)
            after = jnp.where(me < n - 1, rim_r[stage, 1, pl.ds(r + COLS, 64), :], 0.0)
            zf[2, at, :] = jnp.where(low, before, half_roll(zf[8, at, :]))
            zf[2, far, :] = half_roll(jnp.where(low, zf[8, far, :], before))
            zf[11, at, :] = half_roll(jnp.where(low, after, zf[5, at, :]))
            zf[11, far, :] = jnp.where(low, half_roll(zf[5, far, :]), after)
            return carry

        lax.fori_loop(0, COLS // 128, rest, 0)

    def plane_pass(flip, store):
        taps = [pt[3 - a] if flip else pt[a + 3] for a in range(-3, 4)]

        def chunk(i, carry):
            r = pl.multiple_of(i * 64, 64)
            for m in range(PAIRS):
                total = None
                for a in range(-3, 4):
                    term = taps[a + 3] * zf[m + 3 + a, pl.ds(r + (PAD - 2 * a), 64), :]
                    total = term if total is None else total + term
                store(m, r, total)
            return carry

        lax.fori_loop(0, COLS // 64, chunk, 0)

    for m in range(2 * PAIRS):
        zf[m, 0:PAD, :] = jnp.zeros((PAD, LANES), F32)
        zf[m, PAD + COLS : PAD + COLS + PAD, :] = jnp.zeros((PAD, LANES), F32)

    def clear(i, carry):
        for c in range(group):
            lined[pl.ds(c * pitch + 8 * i, 8), :] = jnp.zeros((8, LANES), F32)
        return carry

    loads[0].wait()

    def turn(source, target):
        def one(m, carry):
            for k in range(TILES):
                lanes = slice(k * LANES, (k + 1) * LANES)
                x = jnp.concatenate([source[m, :, lanes], source[m + PAIRS, :, lanes]], axis=0)
                target[m, lanes, :] = x.astype(F32).T
            return carry

        lax.fori_loop(0, PAIRS, one, 0)

    turn(est, est_t)
    send_edges(0, est_t)
    pl.semaphore_wait(barrier, n + 1)
    edges = edge_copies(0)
    for copy in edges:
        copy.start()

    lax.fori_loop(0, PLANES * n // 8, clear, 0)
    for stage in range(2):
        hi, lo = split(row_matrix(rt, stage == 1))
        tmat[stage, 0] = hi
        tmat[stage, 1] = lo
    loads[1].wait()
    for i in range(TILES):
        for j in range(TILES):
            x = w[i * LANES : (i + 1) * LANES, j * LANES : (j + 1) * LANES]
            hi, lo = split(x)
            wmat[1, 0, i * LANES : (i + 1) * LANES, j * LANES : (j + 1) * LANES] = hi
            wmat[1, 1, i * LANES : (i + 1) * LANES, j * LANES : (j + 1) * LANES] = lo
            hi, lo = split(x.T)
            wmat[0, 0, j * LANES : (j + 1) * LANES, i * LANES : (i + 1) * LANES] = hi
            wmat[0, 1, j * LANES : (j + 1) * LANES, i * LANES : (i + 1) * LANES] = lo

    for copy in edges:
        copy.wait()
    join_edges(0)
    row_pass(0, est_t)

    def to_field(m, b, y):
        zf[m + 3, PAD + b * LANES : PAD + (b + 1) * LANES, :] = y

    mix(0, to_field)
    pack_rims(0)
    rims = rim_copies(0)
    for copy in rims:
        copy.start()
    loads[2].wait()
    turn(obs, obs_t)
    for copy in rims:
        copy.wait()
    unpack_rims(0)

    def to_quotient(m, r, total):
        bp[m, pl.ds(r, 64), :] = obs_t[m, pl.ds(r, 64), :] / total

    plane_pass(False, to_quotient)

    def place(i, carry):
        r = pl.multiple_of(i * 64, 64)
        for m in range(PAIRS):
            zf[m + 3, pl.ds(r + PAD, 64), :] = bp[m, pl.ds(r, 64), :]
        return carry

    lax.fori_loop(0, COLS // 64, place, 0)

    pack_rims(1)
    rims = rim_copies(1)
    for copy in rims:
        copy.start()
    for copy in rims:
        copy.wait()
    unpack_rims(1)

    def to_back(m, r, total):
        bp[m, pl.ds(r, 64), :] = total

    plane_pass(True, to_back)
    send_edges(1, bp)
    edges = edge_copies(1)
    for copy in edges:
        copy.start()
    for copy in edges:
        copy.wait()
    join_edges(1)
    row_pass(1, bp)

    def to_updated(m, b, y):
        block = slice(b * LANES, (b + 1) * LANES)
        upd[m, block, :] = est_t[m, block, :] * y

    mix(1, to_updated)

    def first_copy(k):
        dest = lax.rem(me + k, n)
        return pltpu.make_async_remote_copy(
            src_ref=upd.at[:, pl.ds(pl.multiple_of(dest * group, group), group), :],
            dst_ref=got.at[me],
            send_sem=a_ss.at[k],
            recv_sem=a_rs.at[me],
            device_id={"scan": dest, "lat": lat},
            device_id_type=MESH,
        )

    def second_copy(k):
        dest = lax.rem(me + k, n)
        return pltpu.make_async_remote_copy(
            src_ref=back.at[pl.ds(pl.multiple_of(dest * PAIRS * group, 8), PAIRS * group), :],
            dst_ref=fin.at[me],
            send_sem=b_ss.at[k],
            recv_sem=b_rs.at[me],
            device_id={"scan": dest, "lat": lat},
            device_id_type=MESH,
        )

    def start_first(k, carry):
        first_copy(k).start()
        return carry

    lax.fori_loop(1, n, start_first, 0)
    mine = pltpu.make_async_copy(
        upd.at[:, pl.ds(pl.multiple_of(me * group, group), group), :], got.at[me], own_sem.at[0]
    )
    mine.start()
    mine.wait()

    def line_up(s):
        low = lane_ids(8) < ROWS
        for m in range(PAIRS):
            for g in range(group // 8):
                x = got[s, m, 8 * g : 8 * g + 8, :]
                y = half_roll(x)
                start = 8 * g * pitch + PLANES * n + PLANES * s + m
                lined[pl.ds(start, 8, stride=pitch), :] = jnp.where(low, x, y)
                lined[pl.ds(start + PAIRS, 8, stride=pitch), :] = jnp.where(low, y, x)

    line_up(me)

    def take_first(k, carry):
        s = lax.rem(me - k + n, n)
        pltpu.make_async_remote_copy(
            src_ref=upd.at[:, pl.ds(0, group), :],
            dst_ref=got.at[s],
            send_sem=a_ss.at[k],
            recv_sem=a_rs.at[s],
            device_id={"scan": s, "lat": lat},
            device_id_type=MESH,
        ).wait_recv()
        line_up(s)
        return carry

    lax.fori_loop(1, n, take_first, 0)

    def shear(dest):
        low = lane_ids(8) < ROWS
        for c in range(group):
            at = c * pitch + PLANES * n + PLANES * dest - sh[me * group + c]
            x = jnp.where(low, lined[pl.ds(at, 8), :], lined[pl.ds(at + PAIRS, 8), :])
            back[pl.ds(dest * (PAIRS * group) + c, PAIRS, stride=group), :] = x[:PAIRS]

    def start_second(k, carry):
        shear(lax.rem(me + k, n))
        second_copy(k).start()
        return carry

    lax.fori_loop(1, n, start_second, 0)
    shear(me)
    mine = pltpu.make_async_copy(
        back.at[pl.ds(pl.multiple_of(me * PAIRS * group, 8), PAIRS * group), :], fin.at[me], own_sem.at[1]
    )
    mine.start()
    mine.wait()

    def take_second(k, carry):
        s = lax.rem(me - k + n, n)
        pltpu.make_async_remote_copy(
            src_ref=back.at[pl.ds(0, PAIRS * group), :],
            dst_ref=fin.at[s],
            send_sem=b_ss.at[k],
            recv_sem=b_rs.at[s],
            device_id={"scan": s, "lat": lat},
            device_id_type=MESH,
        ).wait_recv()
        return carry

    lax.fori_loop(1, n, take_second, 0)
    per = LANES // group
    for k in range(TILES):
        for m in range(PAIRS):
            x = jnp.concatenate(
                [fin[k * per + j, m * group : (m + 1) * group, :] for j in range(per)], axis=0
            ).T
            outv[m, :, k * LANES : (k + 1) * LANES] = x[:ROWS]
            outv[m + PAIRS, :, k * LANES : (k + 1) * LANES] = x[ROWS:]
    done = pltpu.make_async_copy(outv, out_h, own_sem.at[2])
    done.start()

    def drain(k, carry):
        first_copy(k).wait_send()
        second_copy(k).wait_send()
        return carry

    lax.fori_loop(1, n, drain, 0)
    done.wait()


def solution(mesh):
    n, nl = mesh.shape["scan"], mesh.shape["lat"]
    group = COLS // n
    pitch = 2 * PLANES * n + 9

    def on_device(observed, estimate, column_weights, plane_taps, row_taps, shear_planes):
        any_space = pl.BlockSpec(memory_space=pl.ANY)
        scalars = pl.BlockSpec(memory_space=pltpu.SMEM)
        return pl.pallas_call(
            functools.partial(kernel, n, nl),
            out_shape=jax.ShapeDtypeStruct((PLANES, ROWS, COLS), F32),
            in_specs=[any_space, any_space, any_space, scalars, scalars, scalars],
            out_specs=any_space,
            scratch_shapes=[
                pltpu.VMEM((PLANES, ROWS, COLS), BF16),
                pltpu.VMEM((PLANES, ROWS, COLS), F32),
                pltpu.VMEM((COLS, COLS), F32),
                pltpu.VMEM((PAIRS, COLS, LANES), F32),
                pltpu.VMEM((PAIRS, COLS, LANES), F32),
                pltpu.VMEM((2, 2, COLS, COLS), BF16),
                pltpu.VMEM((2, 2, 2 * LANES, LANES), BF16),
                pltpu.VMEM((2, COLS, LANES), F32),
                pltpu.VMEM((2, 2, COLS, LANES), F32),
                pltpu.VMEM((2, 2, 3 * COLS // 2, LANES), F32),
                pltpu.VMEM((2, 2, 3 * COLS // 2, LANES), F32),
                pltpu.VMEM((COLS, LANES), F32),
                pltpu.VMEM((2 * PAIRS, COLS + 2 * PAD, LANES), F32),
                pltpu.VMEM((PAIRS, COLS, LANES), F32),
                pltpu.VMEM((COLS, PAIRS * LANES), BF16),
                pltpu.VMEM((COLS, PAIRS * LANES), BF16),
                pltpu.VMEM((PAIRS, COLS, LANES), F32),
                pltpu.VMEM((n, PAIRS, group, LANES), F32),
                pltpu.VMEM((group * pitch + 7, LANES), F32),
                pltpu.VMEM((n * PAIRS * group, LANES), F32),
                pltpu.VMEM((n, PAIRS * group, LANES), F32),
                pltpu.VMEM((PLANES, ROWS, COLS), F32),
                pltpu.SemaphoreType.DMA((3,)),
                pltpu.SemaphoreType.DMA((2, 2)),
                pltpu.SemaphoreType.DMA((2, 2)),
                pltpu.SemaphoreType.DMA((2, 2)),
                pltpu.SemaphoreType.DMA((2, 2)),
                pltpu.SemaphoreType.DMA((n,)),
                pltpu.SemaphoreType.DMA((n,)),
                pltpu.SemaphoreType.DMA((n,)),
                pltpu.SemaphoreType.DMA((n,)),
                pltpu.SemaphoreType.DMA((3,)),
            ],
            compiler_params=pltpu.CompilerParams(
                collective_id=0, has_side_effects=True, vmem_limit_bytes=60 * 1024 * 1024
            ),
        )(observed, estimate, column_weights, plane_taps, row_taps, shear_planes)

    placed = (P("scan", "lat", None), P("scan", "lat", None), P(), P(), P(), P())
    return jax.shard_map(
        on_device, mesh=mesh, in_specs=placed, out_specs=P("scan", "lat", None), check_vma=False
    )
```

```python
import functools

import jax
import jax.numpy as jnp
from jax import lax
from jax.experimental import pallas as pl
from jax.experimental.pallas import tpu as pltpu
from jax.sharding import PartitionSpec as P

MESH = pl.DeviceIdType.MESH
F32 = jnp.float32
BF16 = jnp.bfloat16
PLANES = 12
PAIRS = 6
ROWS = 64
COLS = 512
LANES = 128
TILES = COLS // LANES
PAD = 8
HALF = COLS // 2
EDGES = (((0, 320), (320, 512)), ((0, 272), (272, 512)))
RIMS = (((0, 304), (304, 512)), ((0, 288), (288, 512)))
MIXED = (
    (((0, 128), (128, 256), (256, 304)), ((304, 384), (384, 512))),
    (((0, 128), (128, 256)), ((256, 384), (384, 512))),
)


def split(x):
    hi = x.astype(BF16)
    return hi, (x - hi.astype(F32)).astype(BF16)


def dot(a, b):
    return jnp.dot(a, b, preferred_element_type=F32)


def lane_ids(rows):
    return lax.broadcasted_iota(jnp.int32, (rows, LANES), 1)


def half_roll(x):
    return pltpu.roll(x, ROWS, 1)


def row_matrix(taps, flip):
    line = lax.broadcasted_iota(jnp.int32, (LANES, LANES), 0)
    column = lax.broadcasted_iota(jnp.int32, (LANES, LANES), 1)
    same = (line >= ROWS) == (column >= ROWS)
    row = line & (ROWS - 1)
    target = column & (ROWS - 1)
    far = jnp.where(row < ROWS // 2, row + ROWS, row - ROWS)
    own = jnp.zeros((LANES, LANES), F32)
    edge = jnp.zeros((LANES, LANES), F32)
    for b in range(-3, 4):
        tap = taps[3 - b] if flip else taps[b + 3]
        own = jnp.where(same & (row - target == b), tap, own)
        edge = jnp.where(same & (far - target == b), tap, edge)
    return jnp.concatenate([own, edge], axis=0)


def kernel(
    n,
    nl,
    obs_h,
    est_h,
    w_h,
    pt,
    rt,
    sh,
    out_h,
    obs,
    est,
    w,
    est_t,
    obs_t,
    wmat,
    tmat,
    edge_s,
    edge_r,
    rim_s,
    rim_r,
    hc,
    zf,
    zq,
    bp,
    rhi,
    rlo,
    upd,
    got,
    lined,
    back,
    fin,
    outv,
    in_sem,
    edge_ss,
    edge_rs,
    rim_ss,
    rim_rs,
    a_ss,
    a_rs,
    b_ss,
    b_rs,
    own_sem,
):
    group = HALF // n
    pitch = 2 * PLANES * n + 9
    me = lax.axis_index("scan")
    lat = lax.axis_index("lat")
    s_prev, s_next = lax.rem(me + n - 1, n), lax.rem(me + 1, n)
    l_prev, l_next = lax.rem(lat + nl - 1, nl), lax.rem(lat + 1, nl)

    barrier = pltpu.get_barrier_semaphore()

    def greet(k, carry):
        pl.semaphore_signal(barrier, inc=1, device_id={"scan": lax.rem(me + k, n), "lat": lat}, device_id_type=MESH)
        return carry

    for other in (l_prev, l_next):
        pl.semaphore_signal(barrier, inc=1, device_id={"scan": me, "lat": other}, device_id_type=MESH)
    lax.fori_loop(1, n, greet, 0)

    loads = [
        pltpu.make_async_copy(est_h, est, in_sem.at[0]),
        pltpu.make_async_copy(w_h, w, in_sem.at[1]),
        pltpu.make_async_copy(obs_h, obs, in_sem.at[2]),
    ]
    for load in loads:
        load.start()

    def rows_of(lo, hi, body):
        count = (hi - lo) // 64

        def one(i, carry):
            body(pl.multiple_of(lo + i * 64, 8), 64)
            return carry

        if count:
            lax.fori_loop(0, count, one, 0)
        if lo + 64 * count < hi:
            body(lo + 64 * count, hi - lo - 64 * count)

    def send_edges(stage, part, field):
        lo, hi = EDGES[stage][part]

        def chunk(r, size):
            at = pl.ds(r, size)
            lane = lane_ids(size)
            packed = jnp.zeros((size, LANES), F32)
            for m in range(PAIRS):
                x = field[m, at, :]
                moved = pltpu.roll(x, 6 * m, 1) if m else x
                window = (lane + (3 + ROWS - 6 * m)) & (ROWS - 1)
                packed = jnp.where(window < 6, moved, packed)
            edge_s[stage, at, :] = packed

        rows_of(lo, hi, chunk)
        copies = [
            pltpu.make_async_remote_copy(
                src_ref=edge_s.at[stage, lo:hi],
                dst_ref=edge_r.at[stage, i, lo:hi],
                send_sem=edge_ss.at[stage, part, i],
                recv_sem=edge_rs.at[stage, part, i],
                device_id={"scan": me, "lat": other},
                device_id_type=MESH,
            )
            for i, other in ((0, l_next), (1, l_prev))
        ]
        return copies

    def join_edges(stage, part, copies):
        for copy in copies:
            copy.wait_recv()

        def chunk(r, size):
            at = pl.ds(r, size)
            spot = (lane_ids(size) + 3) & (ROWS - 1)
            first = lax.rem(spot, 6) < 3
            before = jnp.where(lat > 0, edge_r[stage, 0, at, :], 0.0)
            after = jnp.where(lat < nl - 1, edge_r[stage, 1, at, :], 0.0)
            hc[at, :] = jnp.where(first, before, after)

        rows_of(*EDGES[stage][part], chunk)

    def row_pass(stage, part, field):
        lo, hi = EDGES[stage][part]
        middle = (lo + hi) // 32 * 16
        for r0, r1 in ((lo, middle), (middle, hi)):
            edges = hc[r0:r1, :]
            for m in range(PAIRS):
                moved = pltpu.roll(edges, LANES - 6 * m, 1) if m else edges
                hi_x, lo_x = split(jnp.concatenate([field[m, r0:r1, :], moved], axis=1))
                t_hi, t_lo = tmat[stage, 0], tmat[stage, 1]
                y_hi, y_lo = split(dot(hi_x, t_hi) + dot(lo_x, t_hi) + dot(hi_x, t_lo))
                rhi[r0:r1, m * LANES : (m + 1) * LANES] = y_hi
                rlo[r0:r1, m * LANES : (m + 1) * LANES] = y_lo

    def mix(stage, blocks, store):
        for r0, r1 in blocks:
            k0, k1 = max(0, r0 - 8) // LANES * LANES, min(COLS, -(-(r1 + 8) // LANES) * LANES)
            w_hi, w_lo = wmat[stage, 0, r0:r1, k0:k1], wmat[stage, 1, r0:r1, k0:k1]
            for pair in range(PAIRS // 2):
                lanes = slice(pair * 2 * LANES, (pair + 1) * 2 * LANES)
                x_hi, x_lo = rhi[k0:k1, lanes], rlo[k0:k1, lanes]
                y = dot(w_hi, x_hi) + dot(w_hi, x_lo) + dot(w_lo, x_hi)
                store(2 * pair, r0, r1, y[:, :LANES])
                store(2 * pair + 1, r0, r1, y[:, LANES:])

    def send_rims(stage, part, zf):
        lo, hi = RIMS[stage][part]
        length = hi - lo
        base = 3 * lo // 2

        def chunk(r, size):
            low = lane_ids(size) < ROWS
            at, to = pl.ds(r + PAD, size), pl.ds(r + (base - lo), size)
            rim_s[stage, 0, to, :] = jnp.where(low, half_roll(zf[6, at, :]), zf[7, at, :])
            rim_s[stage, 1, to, :] = jnp.where(low, zf[3, at, :], half_roll(zf[4, at, :]))

        rows_of(lo, hi, chunk)

        def rest(r, size):
            low = lane_ids(size) < ROWS
            at, far, to = pl.ds(r + PAD, size), pl.ds(r + PAD + length // 2, size), pl.ds(r + (base - lo + length), size)
            rim_s[stage, 0, to, :] = jnp.where(low, half_roll(zf[8, at, :]), zf[8, far, :])
            rim_s[stage, 1, to, :] = jnp.where(low, zf[5, at, :], half_roll(zf[5, far, :]))

        rows_of(lo, lo + length // 2, rest)
        span = slice(base, base + 3 * length // 2)
        copies = [
            pltpu.make_async_remote_copy(
                src_ref=rim_s.at[stage, i, span],
                dst_ref=rim_r.at[stage, i, span],
                send_sem=rim_ss.at[stage, part, i],
                recv_sem=rim_rs.at[stage, part, i],
                device_id={"scan": other, "lat": lat},
                device_id_type=MESH,
            )
            for i, other in ((0, s_next), (1, s_prev))
        ]
        for copy in copies:
            copy.start()
        return copies

    def join_rims(stage, part, copies, zf):
        lo, hi = RIMS[stage][part]
        length = hi - lo
        base = 3 * lo // 2
        for copy in copies:
            copy.wait_recv()

        def chunk(r, size):
            low = lane_ids(size) < ROWS
            at, to = pl.ds(r + PAD, size), pl.ds(r + (base - lo), size)
            before = jnp.where(me > 0, rim_r[stage, 0, to, :], 0.0)
            after = jnp.where(me < n - 1, rim_r[stage, 1, to, :], 0.0)
            zf[0, at, :] = jnp.where(low, before, half_roll(zf[6, at, :]))
            zf[1, at, :] = half_roll(jnp.where(low, zf[7, at, :], before))
            zf[9, at, :] = half_roll(jnp.where(low, after, zf[3, at, :]))
            zf[10, at, :] = jnp.where(low, half_roll(zf[4, at, :]), after)

        rows_of(lo, hi, chunk)

        def rest(r, size):
            low = lane_ids(size) < ROWS
            at, far, to = pl.ds(r + PAD, size), pl.ds(r + PAD + length // 2, size), pl.ds(r + (base - lo + length), size)
            before = jnp.where(me > 0, rim_r[stage, 0, to, :], 0.0)
            after = jnp.where(me < n - 1, rim_r[stage, 1, to, :], 0.0)
            zf[2, at, :] = jnp.where(low, before, half_roll(zf[8, at, :]))
            zf[2, far, :] = half_roll(jnp.where(low, zf[8, far, :], before))
            zf[11, at, :] = half_roll(jnp.where(low, after, zf[5, at, :]))
            zf[11, far, :] = jnp.where(low, half_roll(zf[5, far, :]), after)

        rows_of(lo, lo + length // 2, rest)

    def plane_pass(flip, lo, hi, zf, store):
        taps = [pt[3 - a] if flip else pt[a + 3] for a in range(-3, 4)]

        def chunk(r, size):
            for m in range(PAIRS):
                total = None
                for a in range(-3, 4):
                    term = taps[a + 3] * zf[m + 3 + a, pl.ds(r + (PAD - 2 * a), size), :]
                    total = term if total is None else total + term
                store(m, pl.ds(r, size), total)

        rows_of(lo, hi, chunk)

    for m in range(2 * PAIRS):
        for field in (zf, zq):
            field[m, 0:PAD, :] = jnp.zeros((PAD, LANES), F32)
            field[m, PAD + COLS : PAD + COLS + PAD, :] = jnp.zeros((PAD, LANES), F32)

    def clear(i, carry):
        for c in range(2 * group):
            lined[pl.ds(c * pitch + 8 * i, 8), :] = jnp.zeros((8, LANES), F32)
        return carry

    loads[0].wait()

    def turn(source, target):
        def one(m, carry):
            for k in range(TILES):
                lanes = slice(k * LANES, (k + 1) * LANES)
                x = jnp.concatenate([source[m, :, lanes], source[m + PAIRS, :, lanes]], axis=0)
                target[m, lanes, :] = x.astype(F32).T
            return carry

        lax.fori_loop(0, PAIRS, one, 0)

    turn(est, est_t)
    edges = [send_edges(0, part, est_t) for part in range(2)]
    pl.semaphore_wait(barrier, n + 1)
    for copies in edges:
        for copy in copies:
            copy.start()
    sent = edges[0] + edges[1]

    for stage in range(2):
        hi, lo = split(row_matrix(rt, stage == 1))
        tmat[stage, 0] = hi
        tmat[stage, 1] = lo
    rhi[EDGES[0][0][1] : 3 * LANES, :] = jnp.zeros((3 * LANES - EDGES[0][0][1], PAIRS * LANES), BF16)
    rlo[EDGES[0][0][1] : 3 * LANES, :] = jnp.zeros((3 * LANES - EDGES[0][0][1], PAIRS * LANES), BF16)
    loads[1].wait()
    for i in range(TILES):
        for j in range(TILES):
            x = w[i * LANES : (i + 1) * LANES, j * LANES : (j + 1) * LANES]
            hi, lo = split(x)
            wmat[1, 0, i * LANES : (i + 1) * LANES, j * LANES : (j + 1) * LANES] = hi
            wmat[1, 1, i * LANES : (i + 1) * LANES, j * LANES : (j + 1) * LANES] = lo
            hi, lo = split(x.T)
            wmat[0, 0, j * LANES : (j + 1) * LANES, i * LANES : (i + 1) * LANES] = hi
            wmat[0, 1, j * LANES : (j + 1) * LANES, i * LANES : (i + 1) * LANES] = lo

    def to_field(m, r0, r1, y):
        zf[m + 3, PAD + r0 : PAD + r1, :] = y

    rims = []
    for part in range(2):
        join_edges(0, part, edges[part])
        row_pass(0, part, est_t)
        mix(0, MIXED[0][part], to_field)
        rims.append(send_rims(0, part, zf))
    sent += rims[0] + rims[1]
    loads[2].wait()
    turn(obs, obs_t)
    lax.fori_loop(0, PLANES * n // 8, clear, 0)

    def to_quotient(m, at, total):
        bp[m, at, :] = obs_t[m, at, :] / total

    def place(r, size):
        for m in range(PAIRS):
            zq[m + 3, pl.ds(r + PAD, size), :] = bp[m, pl.ds(r, size), :]

    backs = []
    for part in range(2):
        join_rims(0, part, rims[part], zf)
        plane_pass(False, *RIMS[1][part], zf, to_quotient)
        rows_of(*RIMS[1][part], place)
        backs.append(send_rims(1, part, zq))
    sent += backs[0] + backs[1]

    def to_back(m, at, total):
        bp[m, at, :] = total

    edges = []
    for part in range(2):
        join_rims(1, part, backs[part], zq)
        plane_pass(True, *EDGES[1][part], zq, to_back)
        edges.append(send_edges(1, part, bp))
        for copy in edges[part]:
            copy.start()
    sent += edges[0] + edges[1]

    def to_updated(m, r0, r1, y):
        upd[m, r0:r1, :] = est_t[m, r0:r1, :] * y

    def first_copy(part, k):
        dest = lax.rem(me + k, n)
        return pltpu.make_async_remote_copy(
            src_ref=upd.at[:, pl.ds(pl.multiple_of(part * HALF + dest * group, 8), group), :],
            dst_ref=got.at[part, me],
            send_sem=a_ss.at[part, k],
            recv_sem=a_rs.at[part, me],
            device_id={"scan": dest, "lat": lat},
            device_id_type=MESH,
        )

    def second_copy(part, k):
        dest = lax.rem(me + k, n)
        return pltpu.make_async_remote_copy(
            src_ref=back.at[part, pl.ds(pl.multiple_of(dest * PAIRS * group, 8), PAIRS * group), :],
            dst_ref=fin.at[part, me],
            send_sem=b_ss.at[part, k],
            recv_sem=b_rs.at[part, me],
            device_id={"scan": dest, "lat": lat},
            device_id_type=MESH,
        )

    for part in range(2):
        join_edges(1, part, edges[part])
        row_pass(1, part, bp)
        mix(1, MIXED[1][part], to_updated)

        def start_first(k, carry):
            first_copy(part, k).start()
            return carry

        lax.fori_loop(1, n, start_first, 0)
        mine = pltpu.make_async_copy(
            upd.at[:, pl.ds(pl.multiple_of(part * HALF + me * group, 8), group), :], got.at[part, me], own_sem.at[part]
        )
        mine.start()

    for part in range(2):
        pltpu.make_async_copy(upd.at[:, 0:group, :], got.at[part, me], own_sem.at[part]).wait()

        def line_up(s):
            low = lane_ids(8) < ROWS
            for m in range(PAIRS):
                x = got[part, s, m]
                y = half_roll(x)
                start = part * group * pitch + PLANES * n + PLANES * s + m
                lined[pl.ds(start, group, stride=pitch), :] = jnp.where(low, x, y)
                lined[pl.ds(start + PAIRS, group, stride=pitch), :] = jnp.where(low, y, x)

        line_up(me)

        def take_first(k, carry):
            s = lax.rem(me - k + n, n)
            pltpu.make_async_remote_copy(
                src_ref=upd.at[:, pl.ds(0, group), :],
                dst_ref=got.at[part, s],
                send_sem=a_ss.at[part, k],
                recv_sem=a_rs.at[part, s],
                device_id={"scan": s, "lat": lat},
                device_id_type=MESH,
            ).wait_recv()
            line_up(s)
            return carry

        lax.fori_loop(1, n, take_first, 0)

        def shear(dest):
            low = lane_ids(8) < ROWS
            for c in range(group):
                at = (part * group + c) * pitch + PLANES * n + PLANES * dest - sh[part * HALF + me * group + c]
                x = jnp.where(low, lined[pl.ds(at, 8), :], lined[pl.ds(at + PAIRS, 8), :])
                back[part, pl.ds(dest * (PAIRS * group) + c, PAIRS, stride=group), :] = x[:PAIRS]

        def start_second(k, carry):
            shear(lax.rem(me + k, n))
            second_copy(part, k).start()
            return carry

        lax.fori_loop(1, n, start_second, 0)
        shear(me)
        mine = pltpu.make_async_copy(
            back.at[part, pl.ds(pl.multiple_of(me * PAIRS * group, 8), PAIRS * group), :],
            fin.at[part, me],
            own_sem.at[2 + part],
        )
        mine.start()

    per = LANES // group
    for part in range(2):
        pltpu.make_async_copy(back.at[part, pl.ds(0, PAIRS * group), :], fin.at[part, me], own_sem.at[2 + part]).wait()

        def take_second(k, carry):
            s = lax.rem(me - k + n, n)
            pltpu.make_async_remote_copy(
                src_ref=back.at[part, pl.ds(0, PAIRS * group), :],
                dst_ref=fin.at[part, s],
                send_sem=b_ss.at[part, k],
                recv_sem=b_rs.at[part, s],
                device_id={"scan": s, "lat": lat},
                device_id_type=MESH,
            ).wait_recv()
            return carry

        lax.fori_loop(1, n, take_second, 0)
        for k in range(TILES // 2):
            lanes = slice(part * HALF + k * LANES, part * HALF + (k + 1) * LANES)
            for m in range(PAIRS):
                x = jnp.concatenate(
                    [fin[part, k * per + j, m * group : (m + 1) * group, :] for j in range(per)], axis=0
                ).T
                outv[m, :, lanes] = x[:ROWS]
                outv[m + PAIRS, :, lanes] = x[ROWS:]
        half = slice(part * HALF, (part + 1) * HALF)
        pltpu.make_async_copy(outv.at[:, :, half], out_h.at[:, :, half], own_sem.at[4 + part]).start()

    for copy in sent:
        copy.wait_send()

    def drain(k, carry):
        for part in range(2):
            first_copy(part, k).wait_send()
            second_copy(part, k).wait_send()
        return carry

    lax.fori_loop(1, n, drain, 0)
    for part in range(2):
        half = slice(part * HALF, (part + 1) * HALF)
        pltpu.make_async_copy(outv.at[:, :, half], out_h.at[:, :, half], own_sem.at[4 + part]).wait()

def solution(mesh):
    n, nl = mesh.shape["scan"], mesh.shape["lat"]
    group = HALF // n
    pitch = 2 * PLANES * n + 9

    def on_device(observed, estimate, column_weights, plane_taps, row_taps, shear_planes):
        any_space = pl.BlockSpec(memory_space=pl.ANY)
        scalars = pl.BlockSpec(memory_space=pltpu.SMEM)
        return pl.pallas_call(
            functools.partial(kernel, n, nl),
            out_shape=jax.ShapeDtypeStruct((PLANES, ROWS, COLS), F32),
            in_specs=[any_space, any_space, any_space, scalars, scalars, scalars],
            out_specs=any_space,
            scratch_shapes=[
                pltpu.VMEM((PLANES, ROWS, COLS), BF16),
                pltpu.VMEM((PLANES, ROWS, COLS), F32),
                pltpu.VMEM((COLS, COLS), F32),
                pltpu.VMEM((PAIRS, COLS, LANES), F32),
                pltpu.VMEM((PAIRS, COLS, LANES), F32),
                pltpu.VMEM((2, 2, COLS, COLS), BF16),
                pltpu.VMEM((2, 2, 2 * LANES, LANES), BF16),
                pltpu.VMEM((2, COLS, LANES), F32),
                pltpu.VMEM((2, 2, COLS, LANES), F32),
                pltpu.VMEM((2, 2, 3 * COLS // 2, LANES), F32),
                pltpu.VMEM((2, 2, 3 * COLS // 2, LANES), F32),
                pltpu.VMEM((COLS, LANES), F32),
                pltpu.VMEM((2 * PAIRS, COLS + 2 * PAD, LANES), F32),
                pltpu.VMEM((2 * PAIRS, COLS + 2 * PAD, LANES), F32),
                pltpu.VMEM((PAIRS, COLS, LANES), F32),
                pltpu.VMEM((COLS, PAIRS * LANES), BF16),
                pltpu.VMEM((COLS, PAIRS * LANES), BF16),
                pltpu.VMEM((PAIRS, COLS, LANES), F32),
                pltpu.VMEM((2, n, PAIRS, group, LANES), F32),
                pltpu.VMEM((2 * group * pitch + 7, LANES), F32),
                pltpu.VMEM((2, n * PAIRS * group, LANES), F32),
                pltpu.VMEM((2, n, PAIRS * group, LANES), F32),
                pltpu.VMEM((PLANES, ROWS, COLS), F32),
                pltpu.SemaphoreType.DMA((3,)),
                pltpu.SemaphoreType.DMA((2, 2, 2)),
                pltpu.SemaphoreType.DMA((2, 2, 2)),
                pltpu.SemaphoreType.DMA((2, 2, 2)),
                pltpu.SemaphoreType.DMA((2, 2, 2)),
                pltpu.SemaphoreType.DMA((2, n)),
                pltpu.SemaphoreType.DMA((2, n)),
                pltpu.SemaphoreType.DMA((2, n)),
                pltpu.SemaphoreType.DMA((2, n)),
                pltpu.SemaphoreType.DMA((6,)),
            ],
            compiler_params=pltpu.CompilerParams(
                collective_id=0, has_side_effects=True, vmem_limit_bytes=60 * 1024 * 1024
            ),
        )(observed, estimate, column_weights, plane_taps, row_taps, shear_planes)

    placed = (P("scan", "lat", None), P("scan", "lat", None), P(), P(), P(), P())
    return jax.shard_map(
        on_device, mesh=mesh, in_specs=placed, out_specs=P("scan", "lat", None), check_vma=False
    )
```

```python
import functools

import jax
import jax.numpy as jnp
from jax import lax
from jax.experimental import pallas as pl
from jax.experimental.pallas import tpu as pltpu
from jax.sharding import PartitionSpec as P

MESH = pl.DeviceIdType.MESH
F32 = jnp.float32
BF16 = jnp.bfloat16
PLANES = 12
PAIRS = 6
ROWS = 64
COLS = 512
LANES = 128
TILES = COLS // LANES
PAD = 8
HALF = COLS // 2
PARTS = 4


def ranges(margin):
    ends = [min(COLS, LANES * (part + 1) + margin) for part in range(PARTS - 1)] + [COLS]
    return tuple(zip([0] + ends[:-1], ends))


EDGES = (ranges(64), ranges(16))
RIMS = (ranges(48), ranges(32))
MIXED = (RIMS[0], ranges(0))


def split(x):
    hi = x.astype(BF16)
    return hi, (x - hi.astype(F32)).astype(BF16)


def dot(a, b):
    return jnp.dot(a, b, preferred_element_type=F32)


def lane_ids(rows):
    return lax.broadcasted_iota(jnp.int32, (rows, LANES), 1)


def half_roll(x):
    return pltpu.roll(x, ROWS, 1)


def row_matrix(taps, flip):
    line = lax.broadcasted_iota(jnp.int32, (LANES, LANES), 0)
    column = lax.broadcasted_iota(jnp.int32, (LANES, LANES), 1)
    same = (line >= ROWS) == (column >= ROWS)
    row = line & (ROWS - 1)
    target = column & (ROWS - 1)
    far = jnp.where(row < ROWS // 2, row + ROWS, row - ROWS)
    own = jnp.zeros((LANES, LANES), F32)
    edge = jnp.zeros((LANES, LANES), F32)
    for b in range(-3, 4):
        tap = taps[3 - b] if flip else taps[b + 3]
        own = jnp.where(same & (row - target == b), tap, own)
        edge = jnp.where(same & (far - target == b), tap, edge)
    return jnp.concatenate([own, edge], axis=0)


def kernel(
    n,
    nl,
    obs_h,
    est_h,
    w_h,
    pt,
    rt,
    sh,
    out_h,
    obs,
    est,
    w,
    est_t,
    obs_t,
    wmat,
    tmat,
    edge_s,
    edge_r,
    rim_s,
    rim_r,
    hc,
    zf,
    zq,
    bp,
    rhi,
    rlo,
    upd,
    got,
    lined,
    back,
    fin,
    outv,
    in_sem,
    edge_ss,
    edge_rs,
    rim_ss,
    rim_rs,
    a_ss,
    a_rs,
    b_ss,
    b_rs,
    own_sem,
    far,
):
    group = HALF // n
    share = group // 2
    pitch = 2 * PLANES * n + 9
    me = lax.axis_index("scan")
    lat = lax.axis_index("lat")
    s_prev, s_next = lax.rem(me + n - 1, n), lax.rem(me + 1, n)
    l_prev, l_next = lax.rem(lat + nl - 1, nl), lax.rem(lat + 1, nl)

    barrier = pltpu.get_barrier_semaphore()

    def greet(sem, other):
        pl.semaphore_signal(sem, inc=1, device_id=other, device_id_type=MESH)

    for other in (s_prev, s_next):
        greet(barrier, {"scan": other, "lat": lat})
    for other in (l_prev, l_next):
        greet(barrier, {"scan": me, "lat": other})

    def spread(i, reach):
        for other in (lax.rem(me + n - reach, n), lax.rem(me + reach, n)):
            greet(far.at[i], {"scan": other, "lat": lat})

    def gather(i):
        pl.semaphore_wait(far.at[i], 2)

    loads = [
        pltpu.make_async_copy(est_h, est, in_sem.at[0]),
        pltpu.make_async_copy(w_h, w, in_sem.at[1]),
        pltpu.make_async_copy(obs_h, obs, in_sem.at[2]),
    ]
    for load in loads:
        load.start()

    def rows_of(lo, hi, body):
        count = (hi - lo) // 64

        def one(i, carry):
            body(pl.multiple_of(lo + i * 64, 8), 64)
            return carry

        if count:
            lax.fori_loop(0, count, one, 0)
        if lo + 64 * count < hi:
            body(lo + 64 * count, hi - lo - 64 * count)

    def send_edges(stage, part, field):
        lo, hi = EDGES[stage][part]

        def chunk(r, size):
            at = pl.ds(r, size)
            lane = lane_ids(size)
            packed = jnp.zeros((size, LANES), F32)
            for m in range(PAIRS):
                x = field[m, at, :]
                moved = pltpu.roll(x, 6 * m, 1) if m else x
                window = (lane + (3 + ROWS - 6 * m)) & (ROWS - 1)
                packed = jnp.where(window < 6, moved, packed)
            edge_s[stage, at, :] = packed

        rows_of(lo, hi, chunk)
        copies = [
            pltpu.make_async_remote_copy(
                src_ref=edge_s.at[stage, lo:hi],
                dst_ref=edge_r.at[stage, i, lo:hi],
                send_sem=edge_ss.at[stage, part, i],
                recv_sem=edge_rs.at[stage, part, i],
                device_id={"scan": me, "lat": other},
                device_id_type=MESH,
            )
            for i, other in ((0, l_next), (1, l_prev))
        ]
        return copies

    def join_edges(stage, part, copies):
        for copy in copies:
            copy.wait_recv()

        def chunk(r, size):
            at = pl.ds(r, size)
            spot = (lane_ids(size) + 3) & (ROWS - 1)
            first = lax.rem(spot, 6) < 3
            before = jnp.where(lat > 0, edge_r[stage, 0, at, :], 0.0)
            after = jnp.where(lat < nl - 1, edge_r[stage, 1, at, :], 0.0)
            hc[at, :] = jnp.where(first, before, after)

        rows_of(*EDGES[stage][part], chunk)

    def row_pass(stage, part, field):
        lo, hi = EDGES[stage][part]
        middle = (lo + hi) // 32 * 16
        for r0, r1 in ((lo, middle), (middle, hi)):
            edges = hc[r0:r1, :]
            for m in range(PAIRS):
                moved = pltpu.roll(edges, LANES - 6 * m, 1) if m else edges
                hi_x, lo_x = split(jnp.concatenate([field[m, r0:r1, :], moved], axis=1))
                both = dot(hi_x, tmat[stage, 0])
                y_hi, y_lo = split(both[:, :LANES] + both[:, LANES:] + dot(lo_x, tmat[stage, 0, :, :LANES]))
                rhi[r0:r1, m * LANES : (m + 1) * LANES] = y_hi
                rlo[r0:r1, m * LANES : (m + 1) * LANES] = y_lo

    def mix(stage, part, store):
        r0, r1 = MIXED[stage][part]
        k0, k1 = max(0, r0 - 8) // LANES * LANES, min(COLS, -(-(r1 + 8) // LANES) * LANES)
        w_hi, w_lo = wmat[stage, 0, r0:r1, k0:k1], wmat[stage, 1, r0:r1, k0:k1]
        for pair in range(PAIRS // 2):
            lanes = slice(pair * 2 * LANES, (pair + 1) * 2 * LANES)
            x_hi, x_lo = rhi[k0:k1, lanes], rlo[k0:k1, lanes]
            y = dot(w_hi, x_hi) + dot(w_hi, x_lo) + dot(w_lo, x_hi)
            store(2 * pair, r0, r1, y[:, :LANES])
            store(2 * pair + 1, r0, r1, y[:, LANES:])

    def send_rims(stage, part, zf):
        lo, hi = RIMS[stage][part]
        length = hi - lo
        base = 3 * lo // 2

        def chunk(r, size):
            low = lane_ids(size) < ROWS
            at, to = pl.ds(r + PAD, size), pl.ds(r + (base - lo), size)
            rim_s[stage, 0, to, :] = jnp.where(low, half_roll(zf[6, at, :]), zf[7, at, :])
            rim_s[stage, 1, to, :] = jnp.where(low, zf[3, at, :], half_roll(zf[4, at, :]))

        rows_of(lo, hi, chunk)

        def rest(r, size):
            low = lane_ids(size) < ROWS
            at, far, to = pl.ds(r + PAD, size), pl.ds(r + PAD + length // 2, size), pl.ds(r + (base - lo + length), size)
            rim_s[stage, 0, to, :] = jnp.where(low, half_roll(zf[8, at, :]), zf[8, far, :])
            rim_s[stage, 1, to, :] = jnp.where(low, zf[5, at, :], half_roll(zf[5, far, :]))

        rows_of(lo, lo + length // 2, rest)
        span = slice(base, base + 3 * length // 2)
        copies = [
            pltpu.make_async_remote_copy(
                src_ref=rim_s.at[stage, i, span],
                dst_ref=rim_r.at[stage, i, span],
                send_sem=rim_ss.at[stage, part, i],
                recv_sem=rim_rs.at[stage, part, i],
                device_id={"scan": other, "lat": lat},
                device_id_type=MESH,
            )
            for i, other in ((0, s_next), (1, s_prev))
        ]
        for copy in copies:
            copy.start()
        return copies

    def join_rims(stage, part, copies, zf):
        lo, hi = RIMS[stage][part]
        length = hi - lo
        base = 3 * lo // 2
        for copy in copies:
            copy.wait_recv()

        def chunk(r, size):
            low = lane_ids(size) < ROWS
            at, to = pl.ds(r + PAD, size), pl.ds(r + (base - lo), size)
            before = jnp.where(me > 0, rim_r[stage, 0, to, :], 0.0)
            after = jnp.where(me < n - 1, rim_r[stage, 1, to, :], 0.0)
            zf[0, at, :] = jnp.where(low, before, half_roll(zf[6, at, :]))
            zf[1, at, :] = half_roll(jnp.where(low, zf[7, at, :], before))
            zf[9, at, :] = half_roll(jnp.where(low, after, zf[3, at, :]))
            zf[10, at, :] = jnp.where(low, half_roll(zf[4, at, :]), after)

        rows_of(lo, hi, chunk)

        def rest(r, size):
            low = lane_ids(size) < ROWS
            at, far, to = pl.ds(r + PAD, size), pl.ds(r + PAD + length // 2, size), pl.ds(r + (base - lo + length), size)
            before = jnp.where(me > 0, rim_r[stage, 0, to, :], 0.0)
            after = jnp.where(me < n - 1, rim_r[stage, 1, to, :], 0.0)
            zf[2, at, :] = jnp.where(low, before, half_roll(zf[8, at, :]))
            zf[2, far, :] = half_roll(jnp.where(low, zf[8, far, :], before))
            zf[11, at, :] = half_roll(jnp.where(low, after, zf[5, at, :]))
            zf[11, far, :] = jnp.where(low, half_roll(zf[5, far, :]), after)

        rows_of(lo, lo + length // 2, rest)

    def plane_pass(flip, lo, hi, zf, store):
        taps = [pt[3 - a] if flip else pt[a + 3] for a in range(-3, 4)]

        def chunk(r, size):
            for m in range(PAIRS):
                total = None
                for a in range(-3, 4):
                    term = taps[a + 3] * zf[m + 3 + a, pl.ds(r + (PAD - 2 * a), size), :]
                    total = term if total is None else total + term
                store(m, pl.ds(r, size), total)

        rows_of(lo, hi, chunk)

    for m in range(2 * PAIRS):
        for field in (zf, zq):
            field[m, 0:PAD, :] = jnp.zeros((PAD, LANES), F32)
            field[m, PAD + COLS : PAD + COLS + PAD, :] = jnp.zeros((PAD, LANES), F32)

    def clear(i, carry):
        for c in range(2 * group):
            lined[pl.ds(c * pitch + 8 * i, 8), :] = jnp.zeros((8, LANES), F32)
        return carry

    loads[0].wait()

    def turn(source, target, tiles):
        def one(m, carry):
            for k in tiles:
                lanes = slice(k * LANES, (k + 1) * LANES)
                x = jnp.concatenate([source[m, :, lanes], source[m + PAIRS, :, lanes]], axis=0)
                target[m, lanes, :] = x.astype(F32).T
            return carry

        lax.fori_loop(0, PAIRS, one, 0)

    sent = []
    first_edges = {}

    def open_edges(part):
        first_edges[part] = send_edges(0, part, est_t)
        if part == 0:
            pl.semaphore_wait(barrier, 4)
        for copy in first_edges[part]:
            copy.start()
        sent.extend(first_edges[part])

    def weights(stage):
        for i in range(TILES):
            for j in range(max(0, i - 1), min(TILES, i + 2)):
                rows, columns = slice(i * LANES, (i + 1) * LANES), slice(j * LANES, (j + 1) * LANES)
                hi, lo = split(w[rows, columns] if stage else w[columns, rows].T)
                wmat[stage, 0, rows, columns] = hi
                wmat[stage, 1, rows, columns] = lo
        hi, lo = split(row_matrix(rt, stage == 1))
        tmat[stage, 0, :, :LANES] = hi
        tmat[stage, 0, :, LANES:] = lo

    turn(est, est_t, (0, 1))
    open_edges(0)
    turn(est, est_t, (2, 3))
    for part in range(1, PARTS):
        open_edges(part)
    spread(0, 1)
    loads[1].wait()
    weights(0)
    rest_rows = slice(EDGES[0][0][1], COLS)
    rhi[rest_rows, :] = jnp.zeros((COLS - EDGES[0][0][1], PAIRS * LANES), BF16)
    rlo[rest_rows, :] = jnp.zeros((COLS - EDGES[0][0][1], PAIRS * LANES), BF16)

    def to_field(m, r0, r1, y):
        zf[m + 3, PAD + r0 : PAD + r1, :] = y

    def to_quotient(m, at, total):
        bp[m, at, :] = obs_t[m, at, :] / total

    def place(r, size):
        for m in range(PAIRS):
            zq[m + 3, pl.ds(r + PAD, size), :] = bp[m, pl.ds(r, size), :]

    def to_back(m, at, total):
        bp[m, at, :] = total

    def to_updated(m, r0, r1, y):
        upd[m, r0:r1, :] = est_t[m, r0:r1, :] * y

    def order(k):
        return jnp.where(k == n - 1, k, lax.rem(4 * k, n - 1))

    def first_copy(part, k):
        dest = lax.rem(me + order(k), n)
        return pltpu.make_async_remote_copy(
            src_ref=upd.at[:, pl.ds(pl.multiple_of(part * LANES + dest * share, share), share), :],
            dst_ref=got.at[part // 2, me, :, share * (part % 2) : share * (part % 2 + 1), :],
            send_sem=a_ss.at[part, k],
            recv_sem=a_rs.at[part, me],
            device_id={"scan": dest, "lat": lat},
            device_id_type=MESH,
        )

    def own_first(part):
        return pltpu.make_async_copy(
            upd.at[:, pl.ds(pl.multiple_of(part * LANES + me * share, share), share), :],
            got.at[part // 2, me, :, share * (part % 2) : share * (part % 2 + 1), :],
            own_sem.at[part],
        )

    def second_copy(part, k):
        dest = lax.rem(me + order(k), n)
        return pltpu.make_async_remote_copy(
            src_ref=back.at[part, pl.ds(pl.multiple_of(dest * PAIRS * group, 8), PAIRS * group), :],
            dst_ref=fin.at[part, me],
            send_sem=b_ss.at[part, k],
            recv_sem=b_rs.at[part, me],
            device_id={"scan": dest, "lat": lat},
            device_id_type=MESH,
        )

    rims, backs, last_edges = {}, {}, {}

    def step_field(part):
        join_edges(0, part, first_edges[part])
        row_pass(0, part, est_t)
        mix(0, part, to_field)
        rims[part] = send_rims(0, part, zf)

    def step_quotient(part):
        join_rims(0, part, rims[part], zf)
        plane_pass(False, *RIMS[1][part], zf, to_quotient)
        rows_of(*RIMS[1][part], place)
        backs[part] = send_rims(1, part, zq)

    def step_planes(part):
        join_rims(1, part, backs[part], zq)
        plane_pass(True, *EDGES[1][part], zq, to_back)
        last_edges[part] = send_edges(1, part, bp)
        for copy in last_edges[part]:
            copy.start()

    def step_update(part):
        join_edges(1, part, last_edges[part])
        row_pass(1, part, bp)
        mix(1, part, to_updated)

        def start_first(k, carry):
            first_copy(part, k).start()
            return carry

        lax.fori_loop(1, n, start_first, 0)
        own_first(part).start()

    def prepare():
        loads[2].wait()
        turn(obs, obs_t, range(TILES))

    def tidy():
        lax.fori_loop(0, PLANES * n // 8, clear, 0)

    step_field(0)
    gather(0)
    spread(1, 2)
    prepare()
    step_field(1)
    step_quotient(0)
    gather(1)
    spread(2, 4)
    step_field(2)
    weights(1)
    step_quotient(1)
    step_planes(0)
    gather(2)
    spread(3, 8)
    step_field(3)
    gather(3)
    step_update(0)
    step_quotient(2)
    step_planes(1)
    step_update(1)
    step_quotient(3)
    step_planes(2)
    step_update(2)
    tidy()
    step_planes(3)
    step_update(3)
    for group_of in (rims, backs, last_edges):
        for part in range(PARTS):
            sent += group_of[part]

    for part in range(2):
        own_first(2 * part).wait()
        own_first(2 * part + 1).wait()

        def line_up(s):
            low = lane_ids(8) < ROWS
            for m in range(PAIRS):
                x = got[part, s, m]
                y = half_roll(x)
                start = part * group * pitch + PLANES * n + PLANES * s + m
                lined[pl.ds(start, group, stride=pitch), :] = jnp.where(low, x, y)
                lined[pl.ds(start + PAIRS, group, stride=pitch), :] = jnp.where(low, y, x)

        line_up(me)

        def take_first(k, carry):
            s = lax.rem(me - order(k) + n, n)
            for i in range(2):
                pltpu.make_async_remote_copy(
                    src_ref=upd.at[:, pl.ds(0, share), :],
                    dst_ref=got.at[part, s, :, share * i : share * (i + 1), :],
                    send_sem=a_ss.at[2 * part + i, k],
                    recv_sem=a_rs.at[2 * part + i, s],
                    device_id={"scan": s, "lat": lat},
                    device_id_type=MESH,
                ).wait_recv()
            line_up(s)
            return carry

        lax.fori_loop(1, n, take_first, 0)

        def shear(dest):
            low = lane_ids(8) < ROWS
            for c in range(group):
                at = (part * group + c) * pitch + PLANES * n + PLANES * dest - sh[part * HALF + c // share * LANES + me * share + c % share]
                x = jnp.where(low, lined[pl.ds(at, 8), :], lined[pl.ds(at + PAIRS, 8), :])
                back[part, pl.ds(dest * (PAIRS * group) + c, PAIRS, stride=group), :] = x[:PAIRS]

        def start_second(k, carry):
            shear(lax.rem(me + order(k), n))
            second_copy(part, k).start()
            return carry

        lax.fori_loop(1, n, start_second, 0)
        shear(me)
        mine = pltpu.make_async_copy(
            back.at[part, pl.ds(pl.multiple_of(me * PAIRS * group, 8), PAIRS * group), :],
            fin.at[part, me],
            own_sem.at[4 + part],
        )
        mine.start()

    for part in range(2):
        pltpu.make_async_copy(back.at[part, pl.ds(0, PAIRS * group), :], fin.at[part, me], own_sem.at[4 + part]).wait()

        def take_second(k, carry):
            s = lax.rem(me - order(k) + n, n)
            pltpu.make_async_remote_copy(
                src_ref=back.at[part, pl.ds(0, PAIRS * group), :],
                dst_ref=fin.at[part, s],
                send_sem=b_ss.at[part, k],
                recv_sem=b_rs.at[part, s],
                device_id={"scan": s, "lat": lat},
                device_id_type=MESH,
            ).wait_recv()
            return carry

        lax.fori_loop(1, n, take_second, 0)
        first = lax.broadcasted_iota(jnp.int32, (group, LANES), 0) < share
        for m in range(PAIRS):
            tiles = ([], [])
            for j in range(0, n, 2):
                x = fin[part, j, m * group : (m + 1) * group, :]
                y = fin[part, j + 1, m * group : (m + 1) * group, :]
                tiles[0].append(jnp.where(first, x, pltpu.roll(y, share, 0)))
                tiles[1].append(jnp.where(first, pltpu.roll(x, share, 0), y))
            for k in range(2):
                lanes = slice(part * HALF + k * LANES, part * HALF + (k + 1) * LANES)
                x = jnp.concatenate(tiles[k], axis=0).T
                outv[m, :, lanes] = x[:ROWS]
                outv[m + PAIRS, :, lanes] = x[ROWS:]
            half = slice(part * HALF, (part + 1) * HALF)
            for plane in (m, m + PAIRS):
                pltpu.make_async_copy(
                    outv.at[plane, :, half], out_h.at[plane, :, half], own_sem.at[6 + part]
                ).start()

    for copy in sent:
        copy.wait_send()

    def drain(k, carry):
        for part in range(PARTS):
            first_copy(part, k).wait_send()
        for part in range(2):
            second_copy(part, k).wait_send()
        return carry

    lax.fori_loop(1, n, drain, 0)
    for part in range(2):
        half = slice(part * HALF, (part + 1) * HALF)
        pltpu.make_async_copy(outv.at[:, :, half], out_h.at[:, :, half], own_sem.at[6 + part]).wait()

def solution(mesh):
    n, nl = mesh.shape["scan"], mesh.shape["lat"]
    group = HALF // n
    pitch = 2 * PLANES * n + 9

    def on_device(observed, estimate, column_weights, plane_taps, row_taps, shear_planes):
        any_space = pl.BlockSpec(memory_space=pl.ANY)
        scalars = pl.BlockSpec(memory_space=pltpu.SMEM)
        return pl.pallas_call(
            functools.partial(kernel, n, nl),
            out_shape=jax.ShapeDtypeStruct((PLANES, ROWS, COLS), F32),
            in_specs=[any_space, any_space, any_space, scalars, scalars, scalars],
            out_specs=any_space,
            scratch_shapes=[
                pltpu.VMEM((PLANES, ROWS, COLS), BF16),
                pltpu.VMEM((PLANES, ROWS, COLS), F32),
                pltpu.VMEM((COLS, COLS), F32),
                pltpu.VMEM((PAIRS, COLS, LANES), F32),
                pltpu.VMEM((PAIRS, COLS, LANES), F32),
                pltpu.VMEM((2, 2, COLS, COLS), BF16),
                pltpu.VMEM((2, 1, 2 * LANES, 2 * LANES), BF16),
                pltpu.VMEM((2, COLS, LANES), F32),
                pltpu.VMEM((2, 2, COLS, LANES), F32),
                pltpu.VMEM((2, 2, 3 * COLS // 2, LANES), F32),
                pltpu.VMEM((2, 2, 3 * COLS // 2, LANES), F32),
                pltpu.VMEM((COLS, LANES), F32),
                pltpu.VMEM((2 * PAIRS, COLS + 2 * PAD, LANES), F32),
                pltpu.VMEM((2 * PAIRS, COLS + 2 * PAD, LANES), F32),
                pltpu.VMEM((PAIRS, COLS, LANES), F32),
                pltpu.VMEM((COLS, PAIRS * LANES), BF16),
                pltpu.VMEM((COLS, PAIRS * LANES), BF16),
                pltpu.VMEM((PAIRS, COLS, LANES), F32),
                pltpu.VMEM((2, n, PAIRS, group, LANES), F32),
                pltpu.VMEM((2 * group * pitch + 7, LANES), F32),
                pltpu.VMEM((2, n * PAIRS * group, LANES), F32),
                pltpu.VMEM((2, n, PAIRS * group, LANES), F32),
                pltpu.VMEM((PLANES, ROWS, COLS), F32),
                pltpu.SemaphoreType.DMA((3,)),
                pltpu.SemaphoreType.DMA((2, PARTS, 2)),
                pltpu.SemaphoreType.DMA((2, PARTS, 2)),
                pltpu.SemaphoreType.DMA((2, PARTS, 2)),
                pltpu.SemaphoreType.DMA((2, PARTS, 2)),
                pltpu.SemaphoreType.DMA((PARTS, n)),
                pltpu.SemaphoreType.DMA((PARTS, n)),
                pltpu.SemaphoreType.DMA((2, n)),
                pltpu.SemaphoreType.DMA((2, n)),
                pltpu.SemaphoreType.DMA((8,)),
                pltpu.SemaphoreType.REGULAR((4,)),
            ],
            compiler_params=pltpu.CompilerParams(
                collective_id=0, has_side_effects=True, vmem_limit_bytes=60 * 1024 * 1024
            ),
        )(observed, estimate, column_weights, plane_taps, row_taps, shear_planes)

    placed = (P("scan", "lat", None), P("scan", "lat", None), P(), P(), P(), P())
    return jax.shard_map(
        on_device, mesh=mesh, in_specs=placed, out_specs=P("scan", "lat", None), check_vma=False
    )
```
